32 devices in a mesh: groups: 2 (over y), gx: 4 (over z), gy: 4 (over x, core).
Axes of the slice: x: 2, y: 2, z: 4, core: 2. Of those that a mesh axis runs over, the one named last changes fastest.
Arguments:
- hidden_in: bfloat16 [128, 18432], P(('groups', 'gx'), 'gy'), parts along dimension 0, may hold values from -6 to 6
- w_query: bfloat16 [18432, 12288], P('gy', 'gx'), may hold values from -0.046875 to 0.046875
- w_out: bfloat16 [12288, 18432], P('gx', 'gy'), may hold values from -0.4375 to 0.4375
- cache_keys: bfloat16 [128, 1024, 256], P(('groups', 'gx', 'gy')), parts along dimension 0, may hold values from -250 to 250
- cache_values: bfloat16 [128, 1024, 256], P(('groups', 'gx', 'gy')), parts along dimension 0, may hold values from -6 to 6
- lengths: int32 [128], P(('groups', 'gx', 'gy')), parts along dimension 0, may hold values from 128 to 1024
Outputs:
- layer_out: bfloat16 [128, 18432], P(('groups', 'gx'), 'gy'), parts along dimension 0
The draws below stay inside these ranges and needn't reach their ends.
There are 2 independent parts, one for each index of `groups`. The reference program is written for one: setup_inputs(seed, part) draws one part's arguments, and reference() takes and returns one part's arrays. A program takes and returns all parts, laid end to end along the dimension named above; an argument that names none is the same for every part. Nothing has to cross between parts.
All inputs are finite; a program needn't handle non-finite values.
Results may differ from the reference program's by a relative error of at most 0.0097.
Values may be sent and summed in bfloat16 or wider, within the bound.
No kernel may reach another device: no remote copies, remote signals or barrier semaphores. Data moves between devices by JAX's collectives and lax.ppermute only.
A program may use at most 128 MiB of HBM per device.

```python
import jax
import jax.numpy as jnp
from jax import lax

D = 18432
HEADS = 48
HD = 256
QW = 12288
SEQ_DEV = 4
LMAX = 1024
B = 64


def draw_cache_keys(key, part):
    base = jnp.clip(jax.random.normal(jax.random.fold_in(key, 11), (B, LMAX, HD), jnp.float32), -6.0, 6.0)
    return base.astype(jnp.bfloat16)


def touch_ends(drawn, own_key, smallest, high):
    longest = drawn.shape.index(max(drawn.shape))
    spots = []
    for shift in (0, 1):
        where = [jax.random.randint(jax.random.fold_in(own_key, axis), (), 0, length) for axis, length in enumerate(drawn.shape)]
        where[longest] = (where[longest] + shift) % drawn.shape[longest]
        spots.append(tuple(where))
    return drawn.at[spots[0]].set(smallest).at[spots[1]].set(high)


def levels(own_key, dims, pieces, least, high):
    loudness, own = 1.0, jax.random.fold_in(own_key, 6)
    for dim, shards_of in pieces:
        draws = jnp.exp(jax.random.uniform(jax.random.fold_in(own, dim), (shards_of,), jnp.float32, least / len(pieces), high / len(pieces)))
        loudness = loudness * jnp.repeat(draws, dims[dim] // shards_of).reshape([-1 if axis == dim else 1 for axis in range(len(dims))])
    return loudness


def normal_values(own_key, dims, spread, most, cuts=(), held_as=jnp.bfloat16):
    drawn = jax.random.normal(own_key, dims, jnp.float32) * spread
    if len(cuts) > 0:
        drawn = levels(own_key, dims, cuts, -0.22, 0.18) * drawn
    return jnp.clip(drawn, min=-most, max=most).astype(held_as)


def setup_inputs(seed: int = 0, part: int = 0) -> dict:
    splits = jax.random.split(jax.random.key(seed), 7)
    own_keys = jax.random.split(jax.random.fold_in(splits[6], part), 7)
    return {
        "hidden_in": normal_values(own_keys[0], (B, D), 1.0, 6.0, ((0, 4), (1, 4))),
        "w_query": normal_values(splits[1], (D, QW), D ** -0.5, 0.046875, ((0, 4), (1, 4))),
        "w_out": normal_values(splits[2], (QW, D), (QW // 64) ** -0.5, 0.4375, ((0, 4), (1, 4))),
        "cache_keys": draw_cache_keys(jax.random.fold_in(jax.random.fold_in(splits[6], part), 71), part),
        "cache_values": normal_values(own_keys[4], (B, LMAX, HD), 1.0, 6.0, ((0, 16),)),
        "lengths": touch_ends(jax.random.randint(own_keys[5], (B,), LMAX // 8, LMAX + 1), jax.random.fold_in(own_keys[5], 1), LMAX // 8, LMAX).astype(jnp.int32),
    }


def attend(operands):
    query_block, key_block, value_block, length_block = operands
    scores = jnp.einsum('bhd,bld->bhl', query_block.astype(jnp.float32), key_block.astype(jnp.float32)) / jnp.sqrt(jnp.float32(HD))
    live_slots = jnp.arange(LMAX)[None, None, :] < length_block[:, None, None]
    scores = jnp.where(live_slots, scores, jnp.float32(-1e+30))
    top_score = lax.optimization_barrier(jnp.max(scores, axis=2, keepdims=True))
    expo = jnp.where(live_slots, jnp.exp(scores - top_score), jnp.float32(0.0))
    probs = (expo / lax.optimization_barrier(jnp.sum(expo, axis=2, keepdims=True))).astype(jnp.bfloat16)
    mixed = jnp.einsum('bhl,bld->bhd', probs.astype(jnp.float32), value_block.astype(jnp.float32))
    return mixed.astype(jnp.bfloat16)

def reference(hidden_in, w_query, w_out, cache_keys, cache_values, lengths):
    query = jnp.dot(hidden_in, w_query, preferred_element_type=jnp.float32).astype(jnp.bfloat16)
    blocks = B // SEQ_DEV
    query_heads = query.reshape(blocks, SEQ_DEV, HEADS, HD)
    key_blocks = cache_keys.reshape(blocks, SEQ_DEV, LMAX, HD)
    value_blocks = cache_values.reshape(blocks, SEQ_DEV, LMAX, HD)
    length_blocks = lengths.reshape(blocks, SEQ_DEV)
    attended = lax.map(attend, (query_heads, key_blocks, value_blocks, length_blocks))
    attended = attended.reshape(B, QW)
    return jnp.dot(attended, w_out, preferred_element_type=jnp.float32).astype(jnp.bfloat16)
```

```python
import jax
import jax.numpy as jnp
from jax import lax
from jax.sharding import PartitionSpec as P

NEAR = 8


def shift(x, axis, step):
    size = lax.axis_size(axis)
    return lax.ppermute(x, axis, [(i, (i + step) % size) for i in range(size)])


def exchange(pieces_of, axis):
    size = lax.axis_size(axis)
    me = lax.axis_index(axis)
    return [pieces_of(me)] + [shift(pieces_of((me + s) % size), axis, s) for s in range(1, size)]


def by_source(received, axis):
    size = lax.axis_size(axis)
    me = lax.axis_index(axis)
    stacked = jnp.stack(received[::-1])
    doubled = jnp.concatenate([stacked, stacked])
    return lax.dynamic_slice_in_dim(doubled, (2 * size - me - 1) % size, size, 0)


def gather(x, axis):
    if lax.axis_size(axis) > NEAR:
        return lax.all_gather(x, axis, axis=0)
    return by_source(exchange(lambda dst: x, axis), axis)


def swap(x, axis):
    if lax.axis_size(axis) > NEAR:
        return lax.all_to_all(x, axis, split_axis=0, concat_axis=0)
    pick = lambda dst: lax.dynamic_index_in_dim(x, dst, 0, keepdims=False)
    return by_source(exchange(pick, axis), axis)


def reduce_to(x, axis, sent):
    if lax.axis_size(axis) > NEAR:
        return lax.psum_scatter(x, axis, scatter_dimension=0)
    size = lax.axis_size(axis)
    me = lax.axis_index(axis)
    pick = lambda dst: lax.dynamic_index_in_dim(x, dst, 0, keepdims=False)
    total = pick(me)
    arrived = [shift(pick((me + s) % size).astype(sent), axis, s) for s in range(1, size)]
    for piece in arrived:
        total = total + piece.astype(jnp.float32)
    return total


def parts(width, count):
    count = count if width % (count * 128) == 0 else 1
    return [(i * (width // count), (i + 1) * (width // count)) for i in range(count)]


def dot(a, b):
    return jnp.dot(a, b, preferred_element_type=jnp.float32)


def tiled_product(pieces, w, ks, ns):
    sums = []
    for n0, n1 in ns:
        sums.append(sum(dot(p, w[k0:k1, n0:n1]) for p, (k0, k1) in zip(pieces, ks)))
    return sums


def body(hidden_in, w_query, w_out, cache_keys, cache_values, lengths):
    across = lax.axis_size("gx")
    within = lax.axis_size("gy")
    local_seqs, slot_count, head_dim = cache_keys.shape
    rows = across * within * local_seqs
    slice_width = w_query.shape[1]

    ks = parts(hidden_in.shape[1], 2)
    ns = parts(slice_width, 2)
    pieces = [gather(hidden_in[:, a:b], "gx").reshape(rows, b - a) for a, b in ks]
    owned = []
    for part in tiled_product(pieces, w_query, ks, ns):
        part = part.reshape(across, within, local_seqs, -1).transpose(1, 0, 2, 3)
        owned.append(reduce_to(part, "gy", jnp.float32).astype(jnp.bfloat16))
    owned = jnp.concatenate(owned, axis=2)
    query = swap(owned, "gx").transpose(1, 0, 2).reshape(local_seqs, -1)

    head_count = query.shape[1] // head_dim
    query_heads = query.reshape(local_seqs, head_count, head_dim)
    scores = jnp.einsum("bhd,bld->bhl", query_heads, cache_keys, preferred_element_type=jnp.float32)
    scores = scores / jnp.sqrt(jnp.float32(head_dim))
    live_slots = jnp.arange(slot_count)[None, None, :] < lengths[:, None, None]
    scores = jnp.where(live_slots, scores, jnp.float32(-1e30))
    top_score = jnp.max(scores, axis=2, keepdims=True)
    expo = jnp.where(live_slots, jnp.exp(scores - top_score), jnp.float32(0.0))
    probs = (expo / jnp.sum(expo, axis=2, keepdims=True)).astype(jnp.bfloat16)
    mixed = jnp.einsum("bhl,bld->bhd", probs, cache_values, preferred_element_type=jnp.float32)
    attended = mixed.astype(jnp.bfloat16).reshape(local_seqs, across, slice_width)

    spread = swap(attended.transpose(1, 0, 2), "gx")
    head_rows = gather(spread, "gy").transpose(1, 0, 2, 3).reshape(rows, slice_width)
    ns = parts(w_out.shape[1], 3)
    outs = []
    for (n0, n1) in ns:
        part = dot(head_rows, w_out[:, n0:n1]).reshape(across, within * local_seqs, n1 - n0)
        outs.append(reduce_to(part, "gx", jnp.bfloat16).astype(jnp.bfloat16))
    return jnp.concatenate(outs, axis=1)


def solution(mesh):
    placed = (
        P(("groups", "gx"), "gy"),
        P("gy", "gx"),
        P("gx", "gy"),
        P(("groups", "gx", "gy"), None, None),
        P(("groups", "gx", "gy"), None, None),
        P(("groups", "gx", "gy")),
    )
    return jax.shard_map(
        body, mesh=mesh, in_specs=placed, out_specs=P(("groups", "gx"), "gy"), check_vma=False
    )
```

```python
import jax
import jax.numpy as jnp
from jax import lax
from jax.experimental import pallas as pl
from jax.experimental.pallas import tpu as pltpu
from jax.sharding import PartitionSpec as P

NEAR = 8


def shift(x, axis, step):
    size = lax.axis_size(axis)
    return lax.ppermute(x, axis, [(i, (i + step) % size) for i in range(size)])


def near(axis):
    return lax.axis_size(axis) <= NEAR


def gather(x, axis):
    if not near(axis):
        return lax.all_gather(x, axis, axis=0)
    return jnp.stack([x] + [shift(x, axis, s) for s in range(1, lax.axis_size(axis))])


def swap(x, axis, sign):
    if not near(axis):
        return lax.all_to_all(x, axis, split_axis=0, concat_axis=0)
    return jnp.stack([x[0]] + [shift(x[s], axis, sign * s) for s in range(1, lax.axis_size(axis))])


def reduce_back(x, axis, sent):
    if not near(axis):
        return lax.psum_scatter(x, axis, scatter_dimension=0)
    total = x[0]
    for piece in [shift(x[s].astype(sent), axis, -s) for s in range(1, lax.axis_size(axis))]:
        total = total + piece.astype(jnp.float32)
    return total


def by_source(x, axis):
    if not near(axis):
        return x
    size = lax.axis_size(axis)
    doubled = jnp.concatenate([x[::-1], x[::-1]])
    return lax.dynamic_slice_in_dim(doubled, size - 1 - lax.axis_index(axis), size, 0)


def reduce_to(x, axis):
    if not near(axis):
        return lax.psum_scatter(x, axis, scatter_dimension=0)
    size = lax.axis_size(axis)
    me = lax.axis_index(axis)
    pick = lambda dst: lax.dynamic_index_in_dim(x, dst, 0, keepdims=False)
    total = pick(me)
    for piece in [shift(pick((me + s) % size), axis, s) for s in range(1, size)]:
        total = total + piece
    return total


def parts(width, count):
    count = count if width % (count * 128) == 0 else 1
    return [(i * (width // count), (i + 1) * (width // count)) for i in range(count)]


def product(x, w, k, n, base=None):
    rows, depth = x.shape
    width = n[1] - n[0]
    tile = next(t for t in (512, 384, 256, 128) if width % t == 0 and n[0] % t == 0)
    first = n[0] // tile
    row = k[0] // depth

    def kernel(x_ref, w_ref, *rest):
        acc = jnp.dot(x_ref[...], w_ref[...], preferred_element_type=jnp.float32)
        rest[-1][...] = acc if base is None else acc + rest[0][...]

    in_specs = [
        pl.BlockSpec((rows, depth), lambda j: (0, 0)),
        pl.BlockSpec((depth, tile), lambda j: (row, first + j)),
    ]
    if base is not None:
        in_specs.append(pl.BlockSpec((rows, tile), lambda j: (0, first + j)))
    return pl.pallas_call(
        kernel,
        grid=(width // tile,),
        in_specs=in_specs,
        out_specs=pl.BlockSpec((rows, tile), lambda j: (0, j)),
        out_shape=jax.ShapeDtypeStruct((rows, width), jnp.float32),
        compiler_params=pltpu.CompilerParams(vmem_limit_bytes=40 * 2**20),
    )(x, w, *(() if base is None else (base,)))


def step(hidden_in, w_query, w_out, cache_keys, cache_values, lengths):
    across = lax.axis_size("gx")
    within = lax.axis_size("gy")
    local_seqs, slot_count, head_dim = cache_keys.shape
    rows = across * within * local_seqs
    slice_width = w_query.shape[1]

    k0, k1 = parts(hidden_in.shape[1], 2)
    x0 = gather(hidden_in[:, k0[0]:k0[1]], "gx").reshape(rows, -1)
    x1 = gather(hidden_in[:, k1[0]:k1[1]], "gx").reshape(rows, -1)
    base = product(x0, w_query, k0, (0, slice_width))
    owned = []
    for n in parts(slice_width, 2):
        part = product(x1, w_query, k1, n, base)
        part = part.reshape(across, within, local_seqs, -1).transpose(1, 0, 2, 3)
        owned.append(reduce_to(part, "gy").astype(jnp.bfloat16))
    owned = jnp.concatenate(owned, axis=2)
    query = swap(owned, "gx", -1).transpose(1, 0, 2).reshape(local_seqs, -1)

    head_count = query.shape[1] // head_dim
    query_heads = query.reshape(local_seqs, head_count, head_dim)
    scores = jnp.einsum("bhd,bld->bhl", query_heads, cache_keys, preferred_element_type=jnp.float32)
    scores = scores / jnp.sqrt(jnp.float32(head_dim))
    live_slots = jnp.arange(slot_count)[None, None, :] < lengths[:, None, None]
    scores = jnp.where(live_slots, scores, jnp.float32(-1e30))
    top_score = jnp.max(scores, axis=2, keepdims=True)
    expo = jnp.where(live_slots, jnp.exp(scores - top_score), jnp.float32(0.0))
    probs = (expo / jnp.sum(expo, axis=2, keepdims=True)).astype(jnp.bfloat16)
    mixed = jnp.einsum("bhl,bld->bhd", probs, cache_values, preferred_element_type=jnp.float32)
    attended = mixed.astype(jnp.bfloat16).reshape(local_seqs, across, slice_width)

    spread = swap(attended.transpose(1, 0, 2), "gx", 1)
    head_rows = gather(spread, "gy").transpose(1, 0, 2, 3).reshape(rows, slice_width)
    outs = []
    for n in parts(w_out.shape[1], 3):
        part = product(head_rows, w_out, (0, slice_width), n)
        part = part.reshape(across, within * local_seqs, -1)
        outs.append(reduce_back(part, "gx", jnp.bfloat16).astype(jnp.bfloat16))
    out = jnp.concatenate(outs, axis=1).reshape(within, local_seqs, -1)
    return by_source(out, "gy").reshape(within * local_seqs, -1)


def solution(mesh):
    placed = (
        P(("groups", "gx"), "gy"),
        P("gy", "gx"),
        P("gx", "gy"),
        P(("groups", "gx", "gy"), None, None),
        P(("groups", "gx", "gy"), None, None),
        P(("groups", "gx", "gy")),
    )
    return jax.shard_map(
        step, mesh=mesh, in_specs=placed, out_specs=P(("groups", "gx"), "gy"), check_vma=False
    )
```

```python
import jax
import jax.numpy as jnp
from jax import lax
from jax.experimental import pallas as pl
from jax.experimental.pallas import tpu as pltpu
from jax.sharding import PartitionSpec as P

NEAR = 8


def shift(x, axis, step):
    size = lax.axis_size(axis)
    return lax.ppermute(x, axis, [(i, (i + step) % size) for i in range(size)])


def near(axis):
    return lax.axis_size(axis) <= NEAR


def gather(x, axis):
    if not near(axis):
        return lax.all_gather(x, axis, axis=0)
    return jnp.stack([x] + [shift(x, axis, s) for s in range(1, lax.axis_size(axis))])


def swap(x, axis, sign):
    if not near(axis):
        return lax.all_to_all(x, axis, split_axis=0, concat_axis=0)
    return jnp.stack([x[0]] + [shift(x[s], axis, sign * s) for s in range(1, lax.axis_size(axis))])


def reduce_back(x, axis, sent):
    if not near(axis):
        return lax.psum_scatter(x, axis, scatter_dimension=0)
    total = x[0]
    for piece in [shift(x[s].astype(sent), axis, -s) for s in range(1, lax.axis_size(axis))]:
        total = total + piece.astype(jnp.float32)
    return total


def by_source(x, axis):
    if not near(axis):
        return x
    size = lax.axis_size(axis)
    doubled = jnp.concatenate([x[::-1], x[::-1]])
    return lax.dynamic_slice_in_dim(doubled, size - 1 - lax.axis_index(axis), size, 0)


def reduce_to(x, axis):
    if not near(axis):
        return lax.psum_scatter(x, axis, scatter_dimension=0)
    size = lax.axis_size(axis)
    me = lax.axis_index(axis)
    pick = lambda dst: lax.dynamic_index_in_dim(x, dst, 0, keepdims=False)
    total = pick(me)
    for piece in [shift(pick((me + s) % size), axis, s) for s in range(1, size)]:
        total = total + piece
    return total


def parts(width, count):
    count = count if width % (count * 128) == 0 else 1
    return [(i * (width // count), (i + 1) * (width // count)) for i in range(count)]


def product(x, w, n):
    rows, depth = x.shape
    width = n[1] - n[0]
    tile = next(t for t in (256, 128) if width % t == 0 and n[0] % t == 0)
    first = n[0] // tile

    def kernel(x_ref, w_ref, out_ref):
        out_ref[...] = jnp.dot(x_ref[...], w_ref[...], preferred_element_type=jnp.float32)

    return pl.pallas_call(
        kernel,
        grid=(width // tile,),
        in_specs=[
            pl.BlockSpec((rows, depth), lambda j: (0, 0)),
            pl.BlockSpec((depth, tile), lambda j: (0, first + j)),
        ],
        out_specs=pl.BlockSpec((rows, tile), lambda j: (0, j)),
        out_shape=jax.ShapeDtypeStruct((rows, width), jnp.float32),
        compiler_params=pltpu.CompilerParams(vmem_limit_bytes=40 * 2**20),
    )(x, w)


def step(hidden_in, w_query, w_out, cache_keys, cache_values, lengths):
    across = lax.axis_size("gx")
    within = lax.axis_size("gy")
    local_seqs, slot_count, head_dim = cache_keys.shape
    rows = across * within * local_seqs
    slice_width = w_query.shape[1]

    x = gather(hidden_in, "gx").reshape(across, within, local_seqs, -1)
    x = x.transpose(1, 0, 2, 3).reshape(rows, -1)
    owned = []
    for n in parts(slice_width, 2):
        part = product(x, w_query, n)
        part = part.reshape(within, across * local_seqs, -1)
        owned.append(reduce_to(part, "gy").astype(jnp.bfloat16))
    owned = jnp.concatenate(owned, axis=1).reshape(across, local_seqs, slice_width)
    query = swap(owned, "gx", -1).transpose(1, 0, 2).reshape(local_seqs, -1)

    head_count = query.shape[1] // head_dim
    query_heads = query.reshape(local_seqs, head_count, head_dim)
    scores = jnp.einsum("bhd,bld->bhl", query_heads, cache_keys, preferred_element_type=jnp.float32)
    scores = scores / jnp.sqrt(jnp.float32(head_dim))
    live_slots = jnp.arange(slot_count)[None, None, :] < lengths[:, None, None]
    scores = jnp.where(live_slots, scores, jnp.float32(-1e30))
    top_score = jnp.max(scores, axis=2, keepdims=True)
    expo = jnp.where(live_slots, jnp.exp(scores - top_score), jnp.float32(0.0))
    probs = (expo / jnp.sum(expo, axis=2, keepdims=True)).astype(jnp.bfloat16)
    mixed = jnp.einsum("bhl,bld->bhd", probs, cache_values, preferred_element_type=jnp.float32)
    attended = mixed.astype(jnp.bfloat16).reshape(local_seqs, across, slice_width)

    spread = swap(attended.transpose(1, 0, 2), "gx", 1)
    head_rows = gather(spread, "gy").transpose(1, 0, 2, 3).reshape(rows, slice_width)
    outs = []
    for n in parts(w_out.shape[1], 2):
        part = product(head_rows, w_out, n)
        part = part.reshape(across, within * local_seqs, -1)
        outs.append(reduce_back(part, "gx", jnp.bfloat16).astype(jnp.bfloat16))
    out = jnp.concatenate(outs, axis=1).reshape(within, local_seqs, -1)
    return by_source(out, "gy").reshape(within * local_seqs, -1)


def solution(mesh):
    placed = (
        P(("groups", "gx"), "gy"),
        P("gy", "gx"),
        P("gx", "gy"),
        P(("groups", "gx", "gy"), None, None),
        P(("groups", "gx", "gy"), None, None),
        P(("groups", "gx", "gy")),
    )
    return jax.shard_map(
        step, mesh=mesh, in_specs=placed, out_specs=P(("groups", "gx"), "gy"), check_vma=False
    )
```
